32 devices in a mesh: section: 8 (over z, x), lat: 4 (over y, core).
Axes of the slice: x: 2, y: 2, z: 4, core: 2. Of those that a mesh axis runs over, the one named last changes fastest.
Arguments:
- activations: bfloat16 [8, 2, 64, 8192], P('section', None, None, 'lat'), may hold values from 0.5 to 3
- block_mask: int32 [8, 2, 64], P('section', None, 'lat'), may hold values 0 or 1
- enc_weight: bfloat16 [8, 2304, 8192], P('section', None, 'lat'), may hold values from -0.015625 to 0.015625
- dec_own: bfloat16 [8, 8192, 2304], P('section', 'lat'), may hold values from -0.125 to 0.125
- dec_next: bfloat16 [8, 8192, 2304], P('section', 'lat'), may hold values from -0.125 to 0.125
- grad_seed: float32 [2, 64, 2304], P(None, 'lat'), may hold values from -6 to 6
Outputs:
- residual_grads: float32 [8, 2, 64, 2304], P('section', None, 'lat')
- attribution: bfloat16 [8, 2, 64, 8192], P('section', None, None, 'lat')
The draws below stay inside these ranges and needn't reach their ends.
All inputs are finite; a program needn't handle non-finite values. No bound on the sum of `block_mask` on one device may be relied on, other than what follows from the above.
Results may differ from the reference program's by a relative error of at most 0.01.
Values may be sent and summed in bfloat16 or wider, within the bound.
A program may use at most 64 MiB of HBM per device.

```python
import jax
import jax.numpy as jnp

D = 2304
LAT = 8192
LB = 128
TOK_MB = 64
MB = 2
LAYERS = 8


def set_ends(result, key, low, top_value):
    longest = result.shape.index(max(result.shape))
    spots = []
    for shift in (0, 1):
        where = [jax.random.randint(jax.random.fold_in(key, axis), (), 0, length) for axis, length in enumerate(result.shape)]
        where[longest] = (where[longest] + shift) % result.shape[longest]
        spots.append(tuple(where))
    return result.at[spots[0]].set(low).at[spots[1]].set(top_value)


def block_levels(stream_key, shape, split, least, largest):
    level = 1.0
    for axis_at, shards_of in split:
        heights = jax.random.uniform(jax.random.fold_in(jax.random.fold_in(stream_key, 6), axis_at), (shards_of,), jnp.float32, least / len(split), largest / len(split))
        level = level * jnp.repeat(jnp.exp(heights), shape[axis_at] // shards_of).reshape((-1,) + (1,) * (len(shape) - 1 - axis_at))
    return level


def noise(rng, shape, deviation, most, shards=(), dtype=jnp.bfloat16):
    array = jax.random.normal(rng, shape, jnp.float32) * deviation
    if len(shards) > 0:
        array = block_levels(rng, shape, shards, -0.22, 0.18) * array
    return jnp.clip(array, min=-most, max=most).astype(dtype)


def setup_inputs(seed: int = 0) -> dict:
    seeds = jax.random.split(jax.random.key(seed), 7)
    return {
        "activations": jnp.clip(0.5 + 2.5 * jax.random.uniform(seeds[0], (LAYERS, MB, TOK_MB, LAT), jnp.float32) ** block_levels(seeds[0], (LAYERS, MB, TOK_MB, LAT), ((0, 8), (3, 4)), -0.2, 0.2), 0.5, 3.0).astype(jnp.bfloat16),
        "block_mask": set_ends((jax.random.randint(seeds[1], (LAYERS, MB, LAT // LB), 0, 2) < 1).astype(jnp.int32), jax.random.fold_in(seeds[1], 1), 0, 1),
        "enc_weight": noise(seeds[2], (LAYERS, D, LAT), (16 * LAT) ** -0.5, 0.015625, ((0, 8), (2, 4))),
        "dec_own": noise(seeds[3], (LAYERS, LAT, D), D ** -0.5, 0.125, ((0, 8), (1, 4))),
        "dec_next": noise(seeds[4], (LAYERS, LAT, D), D ** -0.5, 0.125, ((0, 8), (1, 4))),
        "grad_seed": noise(seeds[5], (MB, TOK_MB, D), 1.0, 6.0, ((1, 4),), jnp.float32),
    }


def reference(activations, block_mask, enc_weight, dec_own, dec_next, grad_seed):
    total_rows = MB * TOK_MB
    grad_upper = grad_seed.reshape(total_rows, D)
    above_bf = jnp.zeros((total_rows, D), jnp.bfloat16)
    grads_list = []
    attrib_list = []
    for layer_index in range(LAYERS - 1, -1, -1):
        upper_bf = grad_upper.astype(jnp.bfloat16)
        grad_act = jnp.dot(upper_bf, dec_own[layer_index].T, preferred_element_type=jnp.float32)
        grad_act = grad_act + jnp.dot(above_bf, dec_next[layer_index].T, preferred_element_type=jnp.float32)
        gate_full = jnp.repeat(block_mask[layer_index].astype(jnp.float32), LB, axis=1)
        gate_full = jnp.broadcast_to(gate_full[:, None, :], (MB, TOK_MB, LAT)).reshape(total_rows, LAT)
        active = activations[layer_index].reshape(total_rows, LAT).astype(jnp.float32) * gate_full
        attrib_list.append((active * grad_act).astype(jnp.bfloat16).reshape(MB, TOK_MB, LAT))
        grad_latent = (grad_act * gate_full).astype(jnp.bfloat16)
        grad_lower = grad_upper + jnp.dot(grad_latent, enc_weight[layer_index].T, preferred_element_type=jnp.float32)
        grads_list.append(grad_lower.reshape(MB, TOK_MB, D))
        above_bf = upper_bf
        grad_upper = grad_lower
    return jnp.stack(grads_list[::-1]), jnp.stack(attrib_list[::-1])
```

```python
import functools

import jax
import jax.numpy as jnp
from jax import lax
from jax.experimental import pallas as pl
from jax.experimental.pallas import tpu as pltpu
from jax.sharding import PartitionSpec as P

MESH = pl.DeviceIdType.MESH
NT_DIMS = (((1,), (1,)), ((), ()))


def pick(total, wanted, unit):
    best = unit
    for size in range(unit, wanted + 1, unit):
        if total % size == 0:
            best = size
    return best


def kernel(
    dims, act_hbm, mask_ref, enc_hbm, own_hbm, next_hbm, seed_ref, grads_ref, attr_ref,
    own_w, next_w, enc_w, act, qbuf, abuf, seedq, qout, lo_out, lo_in, psend, pfull, rsbuf, acc, gl, r_up,
    load_sem, rs_send, rs_recv, q_send, q_recv, a_send, a_recv, lo_send, lo_recv,
    qf_send, qf_recv, af_send, af_recv, iq_send, ia_send,
):
    S, N, C, R, D, LATL, PIECES, LT, ET, LOADS, BW = dims
    half = N // 2
    T = N * R
    DP = D // PIECES
    s = lax.axis_index("section")
    j = lax.axis_index("lat")
    partner = j + 1 - 2 * lax.rem(j, 2)
    top = s == S - 1

    def load(array, k):
        src, dst = ((own_hbm, own_w), (enc_hbm, enc_w), (next_hbm, next_w))[array]
        rows = src.shape[0] // LOADS
        part = pl.ds(k * rows, rows)
        return pltpu.make_async_copy(src.at[part], dst.at[part], load_sem.at[array, k])

    act_load = pltpu.make_async_copy(act_hbm, act, load_sem.at[3, 0])
    for array in range(3):
        for k in range(LOADS):
            load(array, k).start()
        if array == 0:
            act_load.start()

    def remote(src, dst, send, recv, section, lat):
        return pltpu.make_async_remote_copy(
            src_ref=src, dst_ref=dst, send_sem=send, recv_sem=recv, device_id=(section, lat), device_id_type=MESH
        )

    def cols(p):
        return pl.ds(p * DP, DP)

    def mate(k):
        return lax.rem(j + 2 * k, N)

    def block(base, k):
        return lax.rem(base + N - 2 * k, N)

    def q_copy(src, send, c, p, k, section):
        return remote(src.at[c, :, cols(p)], qbuf.at[c, j, :, cols(p)], send.at[c, p, k], q_recv.at[c, p, k], section, mate(k))

    def a_copy(src, send, c, k, section):
        return remote(src.at[c], abuf.at[c, j], send.at[c, k], a_recv.at[c, k], section, mate(k))

    def lo_copy(c):
        return remote(lo_out.at[c], lo_in.at[c], lo_send.at[c], lo_recv.at[c], s - 1, j)

    def rs_copy(c, p, k):
        to = lax.rem(j + k, N)
        return remote(psend.at[c, to, :, cols(p)], rsbuf.at[c, k - 1, :, cols(p)], rs_send.at[c, p, k - 1], rs_recv.at[c, p, k - 1], s, to)

    def qf_copy(c, p, k, base):
        at = qbuf.at[c, block(base, k), :, cols(p)]
        return remote(at, at, qf_send.at[c, p, k], qf_recv.at[c, p, k], s, partner)

    def af_copy(c, k, base):
        at = abuf.at[c, block(base, k)]
        return remote(at, at, af_send.at[c, k], af_recv.at[c, k], s, partner)

    barrier = pltpu.get_barrier_semaphore()
    for k in range(1, N):
        pl.semaphore_signal(barrier, inc=1, device_id=(s, lax.rem(j + k, N)), device_id_type=MESH)
    for step in (1, 2):
        for sign in (step, S - step):
            for k in range(half):
                pl.semaphore_signal(barrier, inc=1, device_id=(lax.rem(s + sign, S), mate(k)), device_id_type=MESH)
    pl.semaphore_wait(barrier, (N - 1) + 4 * half)

    @pl.when(top)
    def _():
        for c in range(C):
            seedq[c] = seed_ref[c].astype(jnp.bfloat16)
            for p in range(PIECES):
                for k in range(1, half):
                    q_copy(seedq, iq_send, c, p, k, s).start()
            qbuf[c, j] = seed_ref[c].astype(jnp.bfloat16)
        for c in range(C):
            for k in range(half):
                a_copy(seedq, ia_send, c, k, s - 1).start()

    def chunk(c, carry):
        @pl.when(top)
        def _():
            acc[...] = jnp.zeros_like(acc)
            r_up[...] = seed_ref[c]

        @pl.when(jnp.logical_not(top))
        def _():
            for k in range(half):
                remote(abuf.at[c, block(j, k)], abuf.at[c, block(j, k)], a_send.at[c, k], a_recv.at[c, k], s, partner).wait_recv()
                af_copy(c, k, j).start()

            @pl.when(c == 0)
            def _():
                for k in range(LOADS):
                    load(2, k).wait()

            for k in range(half):
                af_copy(c, k, partner).wait_recv()

            @pl.loop(0, LATL // LT)
            def _(n):
                rows = pl.ds(pl.multiple_of(n * LT, LT), LT)
                above = abuf[c].reshape(T, D)
                acc[n] = lax.dot_general(above, next_w[rows, :], NT_DIMS, preferred_element_type=jnp.float32)

        @pl.when(c == 0)
        def _():
            for k in range(LOADS):
                load(0, k).wait()
            act_load.wait()

        def arrive(p, k):
            at = qbuf.at[c, block(j, k), :, cols(p)]
            remote(at, at, q_send.at[c, p, k], q_recv.at[c, p, k], s, partner).wait_recv()

        for p in range(PIECES):
            pl.when(jnp.logical_not(top))(functools.partial(arrive, p, 0))
            qf_copy(c, p, 0, j).start()
            for k in range(1, half):
                arrive(p, k)
                qf_copy(c, p, k, j).start()
            for k in range(half):
                qf_copy(c, p, k, partner).wait_recv()

            @pl.loop(0, LATL // LT)
            def _(n):
                rows = pl.ds(pl.multiple_of(n * LT, LT), LT)
                upper = qbuf[c, :, :, cols(p)].reshape(T, DP)
                acc[n] += lax.dot_general(upper, own_w[rows, cols(p)], NT_DIMS, preferred_element_type=jnp.float32)

        @pl.loop(0, LATL // LT)
        def _(n):
            for b in range(LT // BW):
                at = pl.ds(pl.multiple_of(n * LT + b * BW, BW), BW)
                gate = mask_ref[c, n * (LT // BW) + b].astype(jnp.float32)
                grad = acc[n, :, b * BW : (b + 1) * BW]
                active = act[c, :, at].astype(jnp.float32) * gate
                attr_ref[c, :, at] = (active * grad).astype(jnp.bfloat16)
                gl[:, at] = (grad * gate).astype(jnp.bfloat16)

        @pl.when(c == 0)
        def _():
            for k in range(LOADS):
                load(1, k).wait()

        for p in range(PIECES):
            @pl.loop(0, DP // ET)
            def _(n):
                at = pl.ds(pl.multiple_of(p * DP + n * ET, ET), ET)
                part = lax.dot_general(gl[...], enc_w[at, :], NT_DIMS, preferred_element_type=jnp.float32)
                part = part.reshape(N, R, ET)
                pfull[:, :, at] = part
                psend[c, :, :, at] = part.astype(jnp.bfloat16)

            for k in range(1, N):
                rs_copy(c, p, k).start()

        @pl.when(jnp.logical_not(top))
        def _():
            lo_copy(c).wait_recv()
            r_up[...] = qbuf[c, j].astype(jnp.float32) + lo_in[c].astype(jnp.float32)

        for p in range(PIECES):
            total = r_up[:, cols(p)] + pfull[j, :, cols(p)]
            for k in range(1, N):
                rs_copy(c, p, k).wait_recv()
                total += rsbuf[c, k - 1, :, cols(p)].astype(jnp.float32)
            grads_ref[c, :, cols(p)] = total
            rounded = total.astype(jnp.bfloat16)
            qout[c, :, cols(p)] = rounded
            lo_out[c, :, cols(p)] = (total - rounded.astype(jnp.float32)).astype(jnp.bfloat16)

            @pl.when(s >= 1)
            def _():
                for k in range(half):
                    q_copy(qout, q_send, c, p, k, s - 1).start()

        @pl.when(s >= 1)
        def _():
            lo_copy(c).start()

        @pl.when(s >= 2)
        def _():
            for k in range(half):
                a_copy(qout, a_send, c, k, s - 2).start()

        return carry

    lax.fori_loop(0, C, chunk, 0)

    @pl.when(top)
    def _():
        for k in range(LOADS):
            load(2, k).wait()
        for c in range(C):
            for p in range(PIECES):
                for k in range(1, half):
                    q_copy(seedq, iq_send, c, p, k, s).wait_send()
            for k in range(half):
                a_copy(seedq, ia_send, c, k, s - 1).wait_send()

    for c in range(C):
        for p in range(PIECES):
            for k in range(1, N):
                rs_copy(c, p, k).wait_send()
            for k in range(half):
                qf_copy(c, p, k, j).wait_send()

    @pl.when(jnp.logical_not(top))
    def _():
        for c in range(C):
            for k in range(half):
                af_copy(c, k, j).wait_send()

    @pl.when(s >= 1)
    def _():
        for c in range(C):
            for p in range(PIECES):
                for k in range(half):
                    q_copy(qout, q_send, c, p, k, s - 1).wait_send()
            lo_copy(c).wait_send()

    @pl.when(s >= 2)
    def _():
        for c in range(C):
            for k in range(half):
                a_copy(qout, a_send, c, k, s - 2).wait_send()


def solution(mesh):
    S, N = mesh.shape["section"], mesh.shape["lat"]

    def local(activations, block_mask, enc_weight, dec_own, dec_next, grad_seed):
        C, T, LATL = activations.shape[1:]
        R, D = grad_seed.shape[1:]
        BW = LATL // block_mask.shape[2]
        half = N // 2
        DP = pick(D, 768, 128)
        PIECES = D // DP
        LT = pick(LATL, 512, BW)
        ET = pick(DP, 256, 128)
        LOADS = 4
        dims = (S, N, C, R, D, LATL, PIECES, LT, ET, LOADS, BW)
        bf, f32 = jnp.bfloat16, jnp.float32
        dma = pltpu.SemaphoreType.DMA
        vmem = pl.BlockSpec(memory_space=pltpu.VMEM)
        smem = pl.BlockSpec(memory_space=pltpu.SMEM)
        hbm = pl.BlockSpec(memory_space=pl.ANY)
        grads, attribution = pl.pallas_call(
            functools.partial(kernel, dims),
            out_shape=(jax.ShapeDtypeStruct((C, R, D), f32), jax.ShapeDtypeStruct((C, T, LATL), bf)),
            in_specs=[hbm, smem, hbm, hbm, hbm, vmem],
            out_specs=(vmem, vmem),
            scratch_shapes=[
                pltpu.VMEM((LATL, D), bf),
                pltpu.VMEM((LATL, D), bf),
                pltpu.VMEM((D, LATL), bf),
                pltpu.VMEM((C, T, LATL), bf),
                pltpu.VMEM((C, N, R, D), bf),
                pltpu.VMEM((C, N, R, D), bf),
                pltpu.VMEM((C, R, D), bf),
                pltpu.VMEM((C, R, D), bf),
                pltpu.VMEM((C, R, D), bf),
                pltpu.VMEM((C, R, D), bf),
                pltpu.VMEM((C, N, R, D), bf),
                pltpu.VMEM((N, R, D), f32),
                pltpu.VMEM((C, N - 1, R, D), bf),
                pltpu.VMEM((LATL // LT, T, LT), f32),
                pltpu.VMEM((T, LATL), bf),
                pltpu.VMEM((R, D), f32),
                dma((4, LOADS)),
                dma((C, PIECES, N - 1)),
                dma((C, PIECES, N - 1)),
                dma((C, PIECES, half)),
                dma((C, PIECES, half)),
                dma((C, half)),
                dma((C, half)),
                dma((C,)),
                dma((C,)),
                dma((C, PIECES, half)),
                dma((C, PIECES, half)),
                dma((C, half)),
                dma((C, half)),
                dma((C, PIECES, half)),
                dma((C, half)),
            ],
            compiler_params=pltpu.CompilerParams(
                collective_id=0, has_side_effects=True, vmem_limit_bytes=56 * 1024 * 1024
            ),
        )(activations[0], block_mask[0], enc_weight[0], dec_own[0], dec_next[0], grad_seed)
        return grads[None], attribution[None]

    placed = (
        P("section", None, None, "lat"),
        P("section", None, "lat"),
        P("section", None, "lat"),
        P("section", "lat", None),
        P("section", "lat", None),
        P(None, "lat", None),
    )
    return jax.shard_map(
        local,
        mesh=mesh,
        in_specs=placed,
        out_specs=(P("section", None, "lat", None), P("section", None, None, "lat")),
        check_vma=False,
    )
```

```python
import functools

import jax
import jax.numpy as jnp
from jax import lax
from jax.experimental import pallas as pl
from jax.experimental.pallas import tpu as pltpu
from jax.sharding import PartitionSpec as P

MESH = pl.DeviceIdType.MESH
NT_DIMS = (((1,), (1,)), ((), ()))
NN_DIMS = (((1,), (0,)), ((), ()))


def pick(total, wanted, unit):
    best = unit
    for size in range(unit, wanted + 1, unit):
        if total % size == 0:
            best = size
    return best


def kernel(
    dims, act_hbm, mask_ref, enc_hbm, own_hbm, next_hbm, seed_ref, grads_ref, attr_ref,
    own_w, next_w, enc_w, own_t, enc_t, act, qbuf, abuf, seedq, qout, lo_out, lo_in, psend, pfull, rsbuf, acc, gl, r_up,
    load_sem, rs_send, rs_recv, q_send, q_recv, a_send, a_recv, lo_send, lo_recv,
    qf_send, qf_recv, af_send, af_recv, iq_send, ia_send,
):
    S, N, C, R, D, LATL, PIECES, LT, ET, TB, LOADS, BW = dims
    half = N // 2
    T = N * R
    DP = D // PIECES
    s = lax.axis_index("section")
    j = lax.axis_index("lat")
    partner = j + 1 - 2 * lax.rem(j, 2)
    top = s == S - 1

    def load(array, k):
        src, dst = ((own_hbm, own_w), (enc_hbm, enc_w), (next_hbm, next_w))[array]
        rows = src.shape[0] // LOADS
        part = pl.ds(k * rows, rows)
        return pltpu.make_async_copy(src.at[part], dst.at[part], load_sem.at[array, k])

    act_load = pltpu.make_async_copy(act_hbm, act, load_sem.at[3, 0])
    for array in range(3):
        for k in range(LOADS):
            load(array, k).start()
        if array == 0:
            act_load.start()

    def remote(src, dst, send, recv, section, lat):
        return pltpu.make_async_remote_copy(
            src_ref=src, dst_ref=dst, send_sem=send, recv_sem=recv, device_id=(section, lat), device_id_type=MESH
        )

    def cols(p):
        return pl.ds(p * DP, DP)

    def mate(k):
        return lax.rem(j + 2 * k, N)

    def block(base, k):
        return lax.rem(base + N - 2 * k, N)

    def q_copy(src, send, c, p, k, section):
        return remote(src.at[c, :, cols(p)], qbuf.at[c, j, :, cols(p)], send.at[c, p, k], q_recv.at[c, p, k], section, mate(k))

    def a_copy(src, send, c, k, section):
        return remote(src.at[c], abuf.at[c, j], send.at[c, k], a_recv.at[c, k], section, mate(k))

    def lo_copy(c):
        return remote(lo_out.at[c], lo_in.at[c], lo_send.at[c], lo_recv.at[c], s - 1, j)

    def rs_copy(c, p, k):
        to = lax.rem(j + k, N)
        return remote(psend.at[c, to, :, cols(p)], rsbuf.at[c, k - 1, :, cols(p)], rs_send.at[c, p, k - 1], rs_recv.at[c, p, k - 1], s, to)

    def qf_copy(c, p, k, base):
        at = qbuf.at[c, block(base, k), :, cols(p)]
        return remote(at, at, qf_send.at[c, p, k], qf_recv.at[c, p, k], s, partner)

    def af_copy(c, k, base):
        at = abuf.at[c, block(base, k)]
        return remote(at, at, af_send.at[c, k], af_recv.at[c, k], s, partner)

    barrier = pltpu.get_barrier_semaphore()
    for k in range(1, N):
        pl.semaphore_signal(barrier, inc=1, device_id=(s, lax.rem(j + k, N)), device_id_type=MESH)
    for step in (1, 2):
        for sign in (step, S - step):
            for k in range(half):
                pl.semaphore_signal(barrier, inc=1, device_id=(lax.rem(s + sign, S), mate(k)), device_id_type=MESH)
    pl.semaphore_wait(barrier, (N - 1) + 4 * half)

    @pl.when(top)
    def _():
        for c in range(C):
            seedq[c] = seed_ref[c].astype(jnp.bfloat16)
            for p in range(PIECES):
                for k in range(1, half):
                    q_copy(seedq, iq_send, c, p, k, s).start()
            qbuf[c, j] = seed_ref[c].astype(jnp.bfloat16)
        for c in range(C):
            for k in range(half):
                a_copy(seedq, ia_send, c, k, s - 1).start()

    @pl.when(jnp.logical_not(top))
    def _():
        for k in range(LOADS):
            load(0, k).wait()

        @pl.loop(0, LATL // LT)
        def _(n):
            @pl.loop(0, D // TB)
            def _(d):
                at = pl.ds(pl.multiple_of(d * TB, TB), TB)
                own_t[n, at, :] = own_w[pl.ds(pl.multiple_of(n * LT, LT), LT), at].T

        for k in range(LOADS):
            load(1, k).wait()

        @pl.loop(0, D // ET)
        def _(e):
            @pl.loop(0, LATL // TB)
            def _(n):
                at = pl.ds(pl.multiple_of(n * TB, TB), TB)
                enc_t[e, at, :] = enc_w[pl.ds(pl.multiple_of(e * ET, ET), ET), at].T

    def chunk(c, carry):
        @pl.when(top)
        def _():
            acc[...] = jnp.zeros_like(acc)
            r_up[...] = seed_ref[c]

        @pl.when(jnp.logical_not(top))
        def _():
            for k in range(half):
                remote(abuf.at[c, block(j, k)], abuf.at[c, block(j, k)], a_send.at[c, k], a_recv.at[c, k], s, partner).wait_recv()
                af_copy(c, k, j).start()

            @pl.when(c == 0)
            def _():
                for k in range(LOADS):
                    load(2, k).wait()

            for k in range(half):
                af_copy(c, k, partner).wait_recv()

            @pl.loop(0, LATL // LT)
            def _(n):
                rows = pl.ds(pl.multiple_of(n * LT, LT), LT)
                above = abuf[c].reshape(T, D)
                acc[n] = lax.dot_general(above, next_w[rows, :], NT_DIMS, preferred_element_type=jnp.float32)

        @pl.when(jnp.logical_and(top, c == 0))
        def _():
            for k in range(LOADS):
                load(0, k).wait()

        def arrive(p, k):
            at = qbuf.at[c, block(j, k), :, cols(p)]
            remote(at, at, q_send.at[c, p, k], q_recv.at[c, p, k], s, partner).wait_recv()

        for p in range(PIECES):
            pl.when(jnp.logical_not(top))(functools.partial(arrive, p, 0))
            qf_copy(c, p, 0, j).start()
            for k in range(1, half):
                arrive(p, k)
                qf_copy(c, p, k, j).start()
            for k in range(half):
                qf_copy(c, p, k, partner).wait_recv()

            @pl.loop(0, LATL // LT)
            def _(n):
                rows = pl.ds(pl.multiple_of(n * LT, LT), LT)
                upper = qbuf[c, :, :, cols(p)].reshape(T, DP)

                @pl.when(top)
                def _():
                    acc[n] += lax.dot_general(upper, own_w[rows, cols(p)], NT_DIMS, preferred_element_type=jnp.float32)

                @pl.when(jnp.logical_not(top))
                def _():
                    acc[n] += lax.dot_general(upper, own_t[n, cols(p), :], NN_DIMS, preferred_element_type=jnp.float32)

        @pl.loop(0, LATL // LT)
        def _(n):
            for b in range(LT // BW):
                at = pl.ds(pl.multiple_of(n * LT + b * BW, BW), BW)
                gate = mask_ref[c, n * (LT // BW) + b].astype(jnp.float32)
                grad = acc[n, :, b * BW : (b + 1) * BW]
                gl[:, at] = (grad * gate).astype(jnp.bfloat16)

        @pl.when(jnp.logical_and(top, c == 0))
        def _():
            for k in range(LOADS):
                load(1, k).wait()

        for p in range(PIECES):
            @pl.loop(0, DP // ET)
            def _(n):
                at = pl.ds(pl.multiple_of(p * DP + n * ET, ET), ET)
                def keep(part):
                    part = part.reshape(N, R, ET)
                    pfull[:, :, at] = part
                    psend[c, :, :, at] = part.astype(jnp.bfloat16)

                @pl.when(top)
                def _():
                    keep(lax.dot_general(gl[...], enc_w[at, :], NT_DIMS, preferred_element_type=jnp.float32))

                @pl.when(jnp.logical_not(top))
                def _():
                    e = p * (DP // ET) + n
                    keep(lax.dot_general(gl[...], enc_t[e], NN_DIMS, preferred_element_type=jnp.float32))

            for k in range(1, N):
                rs_copy(c, p, k).start()

        @pl.when(c == 0)
        def _():
            act_load.wait()

        @pl.loop(0, LATL // LT)
        def _(n):
            for b in range(LT // BW):
                at = pl.ds(pl.multiple_of(n * LT + b * BW, BW), BW)
                gate = mask_ref[c, n * (LT // BW) + b].astype(jnp.float32)
                active = act[c, :, at].astype(jnp.float32) * gate
                attr_ref[c, :, at] = (active * acc[n, :, b * BW : (b + 1) * BW]).astype(jnp.bfloat16)

        @pl.when(jnp.logical_not(top))
        def _():
            lo_copy(c).wait_recv()
            r_up[...] = qbuf[c, j].astype(jnp.float32) + lo_in[c].astype(jnp.float32)

        for p in range(PIECES):
            total = r_up[:, cols(p)] + pfull[j, :, cols(p)]
            for k in range(1, N):
                rs_copy(c, p, k).wait_recv()
                total += rsbuf[c, k - 1, :, cols(p)].astype(jnp.float32)
            rounded = total.astype(jnp.bfloat16)
            qout[c, :, cols(p)] = rounded

            @pl.when(s >= 1)
            def _():
                for k in reversed(range(half)):
                    q_copy(qout, q_send, c, p, k, s - 1).start()

            grads_ref[c, :, cols(p)] = total
            lo_out[c, :, cols(p)] = (total - rounded.astype(jnp.float32)).astype(jnp.bfloat16)

        @pl.when(s >= 1)
        def _():
            lo_copy(c).start()

        @pl.when(s >= 2)
        def _():
            for k in range(half):
                a_copy(qout, a_send, c, k, s - 2).start()

        return carry

    lax.fori_loop(0, C, chunk, 0)

    @pl.when(top)
    def _():
        for k in range(LOADS):
            load(2, k).wait()
        for c in range(C):
            for p in range(PIECES):
                for k in range(1, half):
                    q_copy(seedq, iq_send, c, p, k, s).wait_send()
            for k in range(half):
                a_copy(seedq, ia_send, c, k, s - 1).wait_send()

    for c in range(C):
        for p in range(PIECES):
            for k in range(1, N):
                rs_copy(c, p, k).wait_send()
            for k in range(half):
                qf_copy(c, p, k, j).wait_send()

    @pl.when(jnp.logical_not(top))
    def _():
        for c in range(C):
            for k in range(half):
                af_copy(c, k, j).wait_send()

    @pl.when(s >= 1)
    def _():
        for c in range(C):
            for p in range(PIECES):
                for k in range(half):
                    q_copy(qout, q_send, c, p, k, s - 1).wait_send()
            lo_copy(c).wait_send()

    @pl.when(s >= 2)
    def _():
        for c in range(C):
            for k in range(half):
                a_copy(qout, a_send, c, k, s - 2).wait_send()


def solution(mesh):
    S, N = mesh.shape["section"], mesh.shape["lat"]

    def local(activations, block_mask, enc_weight, dec_own, dec_next, grad_seed):
        C, T, LATL = activations.shape[1:]
        R, D = grad_seed.shape[1:]
        BW = LATL // block_mask.shape[2]
        half = N // 2
        DP = pick(D, 1152, 128)
        PIECES = D // DP
        LT = pick(LATL, 2048, BW)
        ET = pick(DP, 1152, 128)
        TB = 256 if D % 256 == 0 and LATL % 256 == 0 else 128
        LOADS = 4
        dims = (S, N, C, R, D, LATL, PIECES, LT, ET, TB, LOADS, BW)
        bf, f32 = jnp.bfloat16, jnp.float32
        dma = pltpu.SemaphoreType.DMA
        vmem = pl.BlockSpec(memory_space=pltpu.VMEM)
        smem = pl.BlockSpec(memory_space=pltpu.SMEM)
        hbm = pl.BlockSpec(memory_space=pl.ANY)
        grads, attribution = pl.pallas_call(
            functools.partial(kernel, dims),
            out_shape=(jax.ShapeDtypeStruct((C, R, D), f32), jax.ShapeDtypeStruct((C, T, LATL), bf)),
            in_specs=[hbm, smem, hbm, hbm, hbm, vmem],
            out_specs=(vmem, vmem),
            scratch_shapes=[
                pltpu.VMEM((LATL, D), bf),
                pltpu.VMEM((LATL, D), bf),
                pltpu.VMEM((D, LATL), bf),
                pltpu.VMEM((LATL // LT, D, LT), bf),
                pltpu.VMEM((D // ET, LATL, ET), bf),
                pltpu.VMEM((C, T, LATL), bf),
                pltpu.VMEM((C, N, R, D), bf),
                pltpu.VMEM((C, N, R, D), bf),
                pltpu.VMEM((C, R, D), bf),
                pltpu.VMEM((C, R, D), bf),
                pltpu.VMEM((C, R, D), bf),
                pltpu.VMEM((C, R, D), bf),
                pltpu.VMEM((C, N, R, D), bf),
                pltpu.VMEM((N, R, D), f32),
                pltpu.VMEM((C, N - 1, R, D), bf),
                pltpu.VMEM((LATL // LT, T, LT), f32),
                pltpu.VMEM((T, LATL), bf),
                pltpu.VMEM((R, D), f32),
                dma((4, LOADS)),
                dma((C, PIECES, N - 1)),
                dma((C, PIECES, N - 1)),
                dma((C, PIECES, half)),
                dma((C, PIECES, half)),
                dma((C, half)),
                dma((C, half)),
                dma((C,)),
                dma((C,)),
                dma((C, PIECES, half)),
                dma((C, PIECES, half)),
                dma((C, half)),
                dma((C, half)),
                dma((C, PIECES, half)),
                dma((C, half)),
            ],
            compiler_params=pltpu.CompilerParams(
                collective_id=0, has_side_effects=True, vmem_limit_bytes=56 * 1024 * 1024
            ),
        )(activations[0], block_mask[0], enc_weight[0], dec_own[0], dec_next[0], grad_seed)
        return grads[None], attribution[None]

    placed = (
        P("section", None, None, "lat"),
        P("section", None, "lat"),
        P("section", None, "lat"),
        P("section", "lat", None),
        P("section", "lat", None),
        P(None, "lat", None),
    )
    return jax.shard_map(
        local,
        mesh=mesh,
        in_specs=placed,
        out_specs=(P("section", None, "lat", None), P("section", None, None, "lat")),
        check_vma=False,
    )
```
